32 devices in a mesh: row: 4 (over y, core), col: 8 (over z, x).
Axes of the slice: x: 2, y: 2, z: 4, core: 2. Of those that a mesh axis runs over, the one named last changes fastest.
Arguments:
- matrix: float32 [4096, 4096], P('row', 'col'), may hold values from -12 to 12, as said below
Outputs:
- sign_estimate: float32 [4096, 4096], P('row', 'col')
The draws below stay inside these ranges and needn't reach their ends.
Inputs may be any that keep to these rules, and one draw needn't show every extreme that they name: `matrix`: symmetric; the magnitudes of its eigenvalues, divided by the root mean square of all its eigenvalues, lie between 0.4 and 1.7.
All inputs are finite; a program needn't handle non-finite values.
Results may differ from the reference program's by a relative error of at most 0.0002.
Values sent between devices are 32-bit elements; how exact they have to be, the bound alone decides.
A program may use at most 64 MiB of HBM per device.

```python
import math
import jax
import jax.numpy as jnp
from jax import lax

N = 4096
ITERS = 2


def draw_matrix(key, part):
    keys = jax.random.split(jax.random.fold_in(key, 23), 4)
    mixing = 1.0
    factor_low = 0.9
    factor_high = 1.1
    scale_low = 0.25
    scale_high = 4.0
    rough = jax.random.normal(keys[0], (N, N), jnp.float32) * (mixing / math.sqrt(N))
    basis, upper = jnp.linalg.qr(jnp.eye(N, dtype=jnp.float32) + rough)
    place = jnp.arange(N, dtype=jnp.float32) / N
    factor = jax.random.uniform(keys[1], (N,), jnp.float32, factor_low, factor_high)
    signs = jax.random.rademacher(keys[2], (N,), jnp.float32)
    overall = jnp.exp(jax.random.uniform(keys[3], (), jnp.float32, math.log(scale_low), math.log(scale_high)))
    spectrum = signs * (0.6 + 0.9 * place) * factor * overall
    product = jnp.dot(basis * spectrum[None, :], basis.T, precision=lax.Precision.HIGHEST)
    return 0.5 * (product + product.T)


def setup_inputs(seed: int = 0) -> dict:
    arg_keys = jax.random.split(jax.random.key(seed), 2)
    matrix = draw_matrix(jax.random.fold_in(arg_keys[1], 71), 0)
    return dict(matrix=matrix)


def reference(matrix):
    total = jnp.sum(matrix * matrix)
    x_iter = matrix * jnp.sqrt(N / total)
    for step in range(ITERS):
        square = jnp.dot(x_iter.astype(jnp.float32), x_iter.astype(jnp.float32), preferred_element_type=jnp.float32, precision=lax.Precision.HIGHEST)
        cube_block = jnp.dot(x_iter.astype(jnp.float32), square.astype(jnp.float32), preferred_element_type=jnp.float32, precision=lax.Precision.HIGHEST)
        x_iter = 1.5 * x_iter - 0.5 * cube_block
    return x_iter
```

```python
import functools

import jax
import jax.numpy as jnp
from jax import lax
from jax.experimental import pallas as pl
from jax.experimental.pallas import tpu as pltpu
from jax.sharding import PartitionSpec as P

ITERS = 2
MESH = pl.DeviceIdType.MESH
ANY = pl.BlockSpec(memory_space=pl.ANY)
DMA = pltpu.SemaphoreType.DMA
F32, BF16 = jnp.float32, jnp.bfloat16


class Plan:
    def __init__(self, row_n, col_n, block):
        self.row_n, self.col_n = row_n, col_n
        self.h, self.w = block
        self.n = self.h * row_n
        self.ys, self.zs = row_n // 2, col_n // 2
        self.q = self.h // self.w
        self.halved = self.w % 256 == 0
        self.pw = self.w // 2 if self.halved else self.w
        self.pieces = max(2, self.h * self.pw // 32768)
        self.ph = self.h // self.pieces
        self.extra = self.pw // self.ph if self.halved else 0
        self.total = self.pieces + self.extra
        self.split = (self.w // self.ys) % 128 == 0
        self.cw = self.w // self.ys if self.split else self.w

    def locate(self):
        self.row, self.col = lax.axis_index("row"), lax.axis_index("col")
        self.core, self.y = lax.rem(self.row, 2), self.row // 2
        self.x, self.z = lax.rem(self.col, 2), self.col // 2

    def offset(self, row, col, piece):
        if not self.halved:
            return 0
        start = piece * self.ph
        upper = ((row * self.h + start) // self.w < col).astype(jnp.int32)
        return pl.multiple_of(self.pw * lax.rem(start // self.pw + upper, 2), self.pw)

    def place(self, row_block):
        swap = lax.rem(lax.rem(row_block, 2) + self.core, 2)
        return (swap * self.ys + row_block // 2) * self.h

    def is_mine(self, col):
        return lax.rem(col // self.q, 2) == self.core

    def is_diagonal(self, y, col):
        return col // self.q == 2 * y + self.core


def y_steps(plan):
    if plan.ys == 2:
        return ((0, 0), (1, 0))
    return ((0, 0),) + tuple((far, sign) for far in range(1, plan.ys) for sign in (1, -1))


def gather_kernel(plan, x_ref, stage, *rest):
    cross = rest[0] if plan.halved else None
    recv, send, cross_recv, cross_send, keep_sem = rest[-5:]
    plan.locate()
    row, col, core, x, y, z = plan.row, plan.col, plan.core, plan.x, plan.y, plan.z
    partner = row + 1 - 2 * core
    ways = [((row, col + 1 - 2 * x), True)]
    if plan.ys == 2:
        ways.append(((row + 2 - 4 * y, col), True))
    else:
        ways += [((row + 2, col), y < plan.ys - 1), ((row - 2, col), y > 0)]
    ways += [((row, col + 2), z < plan.zs - 1), ((row, col - 2), z > 0)]

    barrier = pltpu.get_barrier_semaphore()
    count = 1
    pl.semaphore_signal(barrier, inc=1, device_id=(partner, col), device_id_type=MESH)
    for target, there in ways:
        if there is True:
            count += 1
            pl.semaphore_signal(barrier, inc=1, device_id=target, device_id_type=MESH)
        else:
            count += there.astype(jnp.int32)

            @pl.when(there)
            def _():
                pl.semaphore_signal(barrier, inc=1, device_id=target, device_id_type=MESH)
    pl.semaphore_wait(barrier, count)

    def own(piece, extra):
        if extra:
            start = lax.rem(col, plan.q) * plan.w + (piece - plan.pieces) * plan.ph
            offset = plan.pw
        else:
            start, offset = piece * plan.ph, plan.offset(row, col, piece)
        return x_ref.at[pl.ds(pl.multiple_of(start, plan.ph), plan.ph), pl.ds(offset, plan.pw)]

    def link(act, way, src, sy, sc, piece):
        dst = stage.at[sy, sc, piece]
        at = sy * plan.col_n + sc
        getattr(pltpu.make_async_remote_copy(
            src_ref=dst if src is None else src, dst_ref=dst, send_sem=send.at[way, at, piece],
            recv_sem=recv.at[at, piece], device_id=ways[way][0], device_id_type=MESH), act)()

    def across(act, src, sy, sc, piece):
        if not plan.halved:
            return
        at = sy * plan.col_n + sc

        @pl.when((piece < plan.pieces) & (lax.rem(sc // plan.q, 2) != core))
        def _():
            getattr(pltpu.make_async_remote_copy(
                src_ref=stage.at[sy, sc, piece] if src is None else src, dst_ref=cross.at[sy, sc, piece],
                send_sem=cross_send.at[at, piece], recv_sem=cross_recv.at[at, piece],
                device_id=(partner, col), device_id_type=MESH), act)()

    def onward(act, src, sy, sc, piece, dx, dy, y_sign, dz, z_sign):
        z_last = piece < plan.pieces // 4
        y_first = lax.rem(piece, 2) == 1
        near = dz == 0
        z_done = jnp.logical_or(jnp.logical_not(z_last), near)

        def go(way, when):
            there = ways[way][1]

            @pl.when(when if there is True else when & there)
            def _():
                link(act, way, src, sy, sc, piece)

        if dx == 0:
            go(0, z_done if dy == 0 else z_done & y_first)
        y_open = z_done if dx == 0 else z_done & jnp.logical_not(y_first)
        if plan.ys == 2:
            if dy == 0:
                go(1, y_open)
        else:
            for way, sign in ((1, -1), (2, 1)):
                if dy == 0 or y_sign == sign:
                    go(way, y_open)
        first = len(ways) - 2
        for way, sign in ((first, -1), (first + 1, 1)):
            here = near | (z_sign == sign)
            go(way, here if dx == 0 and dy == 0 else here & z_last)

    def sweep(act):
        def own_step(extra):
            def step(piece, carry):
                src = own(piece, extra)
                onward(act, src, y, col, piece, 0, 0, 0, jnp.int32(0), 1)
                across(act, src, y, col, piece)
                copy = pltpu.make_async_copy(src, stage.at[y, col, piece], keep_sem.at[piece])
                copy.start() if act == "start" else copy.wait()
                return carry
            return step

        lax.fori_loop(0, plan.pieces, own_step(False), 0)
        if plan.extra:
            @pl.when(plan.is_diagonal(y, col))
            def _():
                lax.fori_loop(plan.pieces, plan.total, own_step(True), 0)

        def event(piece, far, dx, dy, y_sign, z_sign):
            dz = far - dx - dy
            sz = z + z_sign * dz
            sy = 1 - y if plan.ys == 2 and dy else y + y_sign * dy
            sc = 2 * sz + (1 - x if dx else x)
            there = (dz >= (0 if z_sign > 0 else 1)) & (sz >= 0) & (sz < plan.zs)
            if plan.ys != 2:
                there = there & (sy >= 0) & (sy < plan.ys)
            if plan.extra:
                there = there & ((piece < plan.pieces) | plan.is_diagonal(sy, sc))

            @pl.when(there)
            def _():
                if act == "start":
                    dst = stage.at[sy, sc, piece]
                    pltpu.make_async_remote_copy(
                        src_ref=dst, dst_ref=dst, send_sem=send.at[0, 0, 0],
                        recv_sem=recv.at[sy * plan.col_n + sc, piece],
                        device_id=ways[0][0], device_id_type=MESH).wait_recv()
                onward(act, None, sy, sc, piece, dx, dy, y_sign, dz, z_sign)
                across(act, None, sy, sc, piece)

        def round_(far, carry):
            def step(piece, carry):
                for dx in (0, 1):
                    for dy, y_sign in y_steps(plan):
                        for z_sign in (1, -1):
                            event(piece, far, dx, dy, y_sign, z_sign)
                return carry
            return lax.fori_loop(0, plan.total, step, carry)

        lax.fori_loop(1, plan.zs + plan.ys, round_, 0)

    sweep("start")
    sweep("wait_send" if True else None)
    if plan.halved:
        def last(at, carry):
            sy, sc = at // plan.col_n, lax.rem(at, plan.col_n)

            @pl.when(plan.is_mine(sc))
            def _():
                def step(piece, carry):
                    dst = cross.at[sy, sc, piece]
                    pltpu.make_async_remote_copy(
                        src_ref=dst, dst_ref=dst, send_sem=cross_send.at[0, 0], recv_sem=cross_recv.at[at, piece],
                        device_id=(partner, col), device_id_type=MESH).wait_recv()
                    return carry
                lax.fori_loop(0, plan.pieces, step, 0)
            return carry
        lax.fori_loop(0, plan.ys * plan.col_n, last, 0)


def gather(plan, x):
    full = (plan.ys, plan.col_n)
    shapes = [jax.ShapeDtypeStruct((*full, plan.total, plan.ph, plan.pw), F32)]
    if plan.halved:
        shapes.append(jax.ShapeDtypeStruct((*full, plan.pieces, plan.ph, plan.pw), F32))
    count = plan.ys * plan.col_n
    ways = 4 if plan.ys == 2 else 5
    return pl.pallas_call(
        functools.partial(gather_kernel, plan),
        out_shape=shapes, in_specs=[ANY], out_specs=[ANY] * len(shapes),
        scratch_shapes=[DMA((count, plan.total)), DMA((ways, count, plan.total)), DMA((count, plan.pieces)),
                        DMA((count, plan.pieces)), DMA((plan.total,))],
        compiler_params=pltpu.CompilerParams(collective_id=0, has_side_effects=True),
        name="gather",
    )(x)


STEPS = 8


def weights(step):
    def pick(table, other):
        value = jnp.float32(other)
        for at, entry in table:
            value = jnp.where(step == at, jnp.float32(entry), value)
        return value
    return (pick(((1, 1.5), (7, 1.5)), 0.0), pick(((4, 1.5), (7, -0.75)), 0.0),
            pick(((1, -0.5), (4, -0.5), (7, 0.25)), 1.0))


def apply_kernel(plan, stage, *rest):
    if plan.halved:
        cross, rest = rest[0], rest[1:]
    (out, high, low, own_high, own_low, peer_high, peer_low, panel, peer, first, second, loaded, squares, peer_squares,
     scale, load_sem, panel_send, panel_recv, square_sems, out_local, out_send, out_recv) = rest
    plan.locate()
    row, col, core, x, y, z = plan.row, plan.col, plan.core, plan.x, plan.y, plan.z
    h, w, q, ph, pw, half, cw = plan.h, plan.w, plan.q, plan.ph, plan.pw, plan.n // 2, plan.cw
    partner = (row + 1 - 2 * core, col)

    barrier = pltpu.get_barrier_semaphore()
    pl.semaphore_signal(barrier, inc=1, device_id=partner, device_id_type=MESH)
    if plan.split:
        for far in range(1, plan.ys):
            pl.semaphore_signal(barrier, inc=1, device_id=(2 * lax.rem(y + far, plan.ys) + core, col), device_id_type=MESH)
    pl.semaphore_wait(barrier, plan.ys if plan.split else 1)

    def put(tile, at, to):
        top = tile.astype(BF16)
        rest = (tile - top.astype(F32)).astype(BF16)
        rows = pl.ds(pl.multiple_of(at, tile.shape[0]), tile.shape[0])
        cols = pl.ds(pl.multiple_of(to, tile.shape[1]), tile.shape[1])
        high[rows, cols] = top
        low[rows, cols] = rest
        both = tile * tile
        squares[...] += jnp.sum(both.reshape(tile.shape[0] // 8, 8, tile.shape[1] // 128, 128), axis=(0, 2))

    def put_direct(tile, sy, sc, piece):
        put(tile, sy * h + piece * ph, plan.place(sc // q) + lax.rem(sc, q) * w + plan.offset(2 * sy + core, sc, piece))

    def put_turned(tile, sy, core_from, sc, piece):
        source = 2 * sy + core_from
        at = (sc // q // 2) * h + lax.rem(sc, q) * w + plan.offset(source, sc, piece)
        put(tile.T, at, plan.place(source) + piece * ph)

    squares[...] = jnp.zeros_like(squares)

    def streamed(count, source, use):
        def fetch(at):
            slot = lax.rem(at, 2)
            return pltpu.make_async_copy(source(at), loaded.at[slot], load_sem.at[slot])
        fetch(0).start()

        def step(at, carry):
            @pl.when(at + 1 < count)
            def _():
                fetch(at + 1).start()
            fetch(at).wait()
            use(at, loaded.at[lax.rem(at, 2)])
            return carry
        lax.fori_loop(0, count, step, 0)

    def stage_of(at):
        return stage.at[at // plan.col_n, lax.rem(at, plan.col_n), pl.ds(0, plan.pieces)]

    def use_stage(at, ref):
        sy, sc = at // plan.col_n, lax.rem(at, plan.col_n)

        def step(piece, carry):
            put_direct(ref[piece], sy, sc, piece)
            if plan.halved:
                block = ((2 * sy + core) * h + piece * ph) // w

                @pl.when(plan.is_mine(sc) & (block != sc))
                def _():
                    put_turned(ref[piece], sy, core, sc, piece)
            return carry
        lax.fori_loop(0, plan.pieces, step, 0)

    streamed(plan.ys * plan.col_n, stage_of, use_stage)

    if plan.halved:
        def mine(at):
            u = lax.rem(at, plan.col_n // 2)
            return at // (plan.col_n // 2), (2 * (u // q) + core) * q + lax.rem(u, q)

        def use_cross(at, ref):
            sy, sc = mine(at)

            def step(piece, carry):
                put_turned(ref[piece], sy, 1 - core, sc, piece)
                return carry
            lax.fori_loop(0, plan.pieces, step, 0)

        def cross_of(at):
            sy, sc = mine(at)
            return cross.at[sy, sc]

        streamed(plan.ys * plan.col_n // 2, cross_of, use_cross)

        def diagonal(at, carry):
            sy = at // q
            sc = q * (2 * sy + core) + lax.rem(at, q)
            some = loaded.at[0, pl.ds(0, plan.extra)]
            copy = pltpu.make_async_copy(stage.at[sy, sc, pl.ds(plan.pieces, plan.extra)], some, load_sem.at[0])
            copy.start()
            copy.wait()
            corner = sy * h + lax.rem(sc, q) * w
            base = plan.place(sc // q) + lax.rem(sc, q) * w
            for e in range(plan.extra):
                tile = loaded[0, e]
                put(tile, corner + e * ph, base + pw)
                put(tile.T, corner + pw, base + e * ph)
            return carry
        lax.fori_loop(0, plan.ys * q, diagonal, 0)

    share = pltpu.make_async_remote_copy(src_ref=squares, dst_ref=peer_squares, send_sem=square_sems.at[0],
                                         recv_sem=square_sems.at[1], device_id=partner, device_id_type=MESH)
    share.start()
    share.wait()
    total = jnp.sum(jnp.sum(squares[...] + peer_squares[...], axis=0, keepdims=True), axis=1, keepdims=True)
    scale[...] = jnp.broadcast_to(jnp.sqrt(plan.n / total), scale.shape)

    def send(slot, tile):
        rows = pl.ds(pl.multiple_of(tile * h, h), h)
        return pltpu.make_async_remote_copy(
            src_ref=panel.at[slot, rows], dst_ref=peer.at[slot, rows], send_sem=panel_send.at[slot, tile],
            recv_sem=panel_recv.at[slot, tile], device_id=partner, device_id_type=MESH)

    def parts(value):
        top = value.astype(BF16)
        return top, (value - top.astype(F32)).astype(BF16)

    start = plan.place(col // q) + lax.rem(col, q) * w + (y * cw if plan.split else 0)
    mine_cols = pl.ds(pl.multiple_of(start, cw), cw)

    def begin(tile, carry):
        rows = pl.ds(pl.multiple_of(tile * h, h), h)
        value = scale[0:1, 0:1] * (high[rows, mine_cols].astype(F32) + low[rows, mine_cols].astype(F32))
        first[rows, :] = value
        second[rows, :] = value
        panel[0, rows] = value
        own_high[rows, :], own_low[rows, :] = parts(value)
        send(0, tile).start()
        return carry
    lax.fori_loop(0, plan.ys, begin, 0)

    def product(rows, cols, b_high, b_low):
        a_high, a_low = high[rows, cols], low[rows, cols]
        top = b_high[...]
        acc = jnp.dot(a_high, top, preferred_element_type=F32)
        acc += jnp.dot(a_high, b_low[...], preferred_element_type=F32)
        return acc + jnp.dot(a_low, top, preferred_element_type=F32)

    def deliver(act):
        for far in range(1, plan.ys):
            to = lax.rem(y + far, plan.ys)
            copy = pltpu.make_async_remote_copy(
                src_ref=panel.at[STEPS % 2, pl.ds(pl.multiple_of(to * h, h), h)],
                dst_ref=out.at[:, pl.ds(pl.multiple_of(y * cw, cw), cw)],
                send_sem=out_send.at[far - 1], recv_sem=out_recv.at[far - 1],
                device_id=(2 * to + core, col), device_id_type=MESH)
            getattr(copy, act)()

    def step_(step, carry):
        now, later = lax.rem(step, 2), lax.rem(step + 1, 2)

        @pl.when(step > 0)
        def _():
            for tile in range(plan.ys):
                send(later, tile).wait_send()

        def near(tile, carry):
            rows = pl.ds(pl.multiple_of(tile * h, h), h)
            panel[later, rows] = product(rows, slice(0, half), own_high, own_low)
            return carry
        lax.fori_loop(0, plan.ys, near, 0)

        for tile in range(plan.ys):
            send(now, tile).wait_recv()
        peer_high[...], peer_low[...] = parts(peer[now])
        a, b, c = weights(step)

        def far(at, carry):
            tile = lax.rem(y + 1 + at, plan.ys)
            rows = pl.ds(pl.multiple_of(tile * h, h), h)
            value = scale[0:1, 0:1] * (panel[later, rows] + product(rows, slice(half, 2 * half), peer_high, peer_low))
            value = a * first[rows, :] + b * second[rows, :] + c * value
            panel[later, rows] = value
            own_high[rows, :], own_low[rows, :] = parts(value)

            @pl.when(step == 1)
            def _():
                first[rows, :] = value

            @pl.when((step == 2) | (step == 5))
            def _():
                second[rows, :] = value

            @pl.when(step < STEPS - 1)
            def _():
                send(later, tile).start()
            return carry
        lax.fori_loop(0, plan.ys, far, 0)
        return carry
    lax.fori_loop(0, STEPS, step_, 0)
    for tile in range(plan.ys):
        send((STEPS - 1) % 2, tile).wait_send()

    local = pltpu.make_async_copy(
        panel.at[STEPS % 2, pl.ds(pl.multiple_of(y * h, h), h)],
        out.at[:, pl.ds(pl.multiple_of(y * cw if plan.split else 0, cw), cw)], out_local)
    local.start()
    if plan.split:
        deliver("start")
        deliver("wait")
    local.wait()


def apply(plan, staged):
    h, half, cw = plan.h, plan.n // 2, plan.cw
    vmem = pltpu.VMEM
    return pl.pallas_call(
        functools.partial(apply_kernel, plan),
        out_shape=jax.ShapeDtypeStruct((h, plan.w), F32), in_specs=[ANY] * len(staged), out_specs=ANY,
        scratch_shapes=[vmem((half, plan.n), BF16)] * 2 + [vmem((half, cw), BF16)] * 4
        + [vmem((2, half, cw), F32)] * 2 + [vmem((half, cw), F32)] * 2
        + [vmem((2, plan.pieces, plan.ph, plan.pw), F32), vmem((8, 128), F32), vmem((8, 128), F32), vmem((8, 128), F32),
           DMA((2,)), DMA((2, plan.ys)), DMA((2, plan.ys)), DMA((2,)), DMA(()), DMA((plan.ys - 1,)), DMA((plan.ys - 1,))],
        compiler_params=pltpu.CompilerParams(collective_id=1, has_side_effects=True, vmem_limit_bytes=63 * 2**20),
        name="apply",
    )(*staged)


def shards(row_n, col_n, matrix):
    plan = Plan(row_n, col_n, matrix.shape)
    return apply(plan, gather(plan, matrix))


def solution(mesh):
    body = functools.partial(shards, mesh.shape["row"], mesh.shape["col"])
    return jax.shard_map(body, mesh=mesh, in_specs=(P("row", "col"),), out_specs=P("row", "col"), check_vma=False)
```

```python
import functools

import jax
import jax.numpy as jnp
from jax import lax
from jax.experimental import pallas as pl
from jax.experimental.pallas import tpu as pltpu
from jax.sharding import PartitionSpec as P

ITERS = 2
MESH = pl.DeviceIdType.MESH
ANY = pl.BlockSpec(memory_space=pl.ANY)
DMA = pltpu.SemaphoreType.DMA
F32, BF16 = jnp.float32, jnp.bfloat16


class Plan:
    def __init__(self, row_n, col_n, block):
        self.row_n, self.col_n = row_n, col_n
        self.h, self.w = block
        self.n = self.h * row_n
        self.ys, self.zs = row_n // 2, col_n // 2
        self.q = self.h // self.w
        self.halved = self.w % 256 == 0
        self.pw = self.w // 2 if self.halved else self.w
        self.pieces = max(2, self.h * self.pw // 32768)
        self.ph = self.h // self.pieces
        self.extra = self.pw // self.ph if self.halved else 0
        self.total = self.pieces + self.extra
        self.split = (self.w // self.ys) % 128 == 0
        self.cw = self.w // self.ys if self.split else self.w

    def locate(self):
        self.row, self.col = lax.axis_index("row"), lax.axis_index("col")
        self.core, self.y = lax.rem(self.row, 2), self.row // 2
        self.x, self.z = lax.rem(self.col, 2), self.col // 2

    def offset(self, row, col, piece):
        if not self.halved:
            return 0
        start = piece * self.ph
        upper = ((row * self.h + start) // self.w < col).astype(jnp.int32)
        return pl.multiple_of(self.pw * lax.rem(start // self.pw + upper, 2), self.pw)

    def place(self, row_block):
        swap = lax.rem(lax.rem(row_block, 2) + self.core, 2)
        return (swap * self.ys + row_block // 2) * self.h

    def is_mine(self, col):
        return lax.rem(col // self.q, 2) == self.core

    def is_diagonal(self, y, col):
        return col // self.q == 2 * y + self.core


def places(plan):
    ys = ((0, 0), (1, 0)) if plan.ys == 2 else ((0, 0),) + tuple(
        (far, sign) for far in range(1, plan.ys) for sign in (1, -1))
    return [(dx, dy, y_sign, z_sign) for dx in (0, 1) for dy, y_sign in ys for z_sign in (1, -1)]


class Gather:
    def __init__(self, plan, x_ref, stage, cross, put, tiles, turned, sems):
        self.plan, self.x_ref, self.stage, self.cross, self.put = plan, x_ref, stage, cross, put
        self.tiles, self.turned = tiles, turned
        self.recv, self.send, self.cross_recv, self.cross_send, self.tile_sem, self.turned_sem = sems
        row, col, x, y, z = plan.row, plan.col, plan.x, plan.y, plan.z
        self.partner = (row + 1 - 2 * plan.core, col)
        self.ways = [((row, col + 1 - 2 * x), True)]
        if plan.ys == 2:
            self.ways.append(((row + 2 - 4 * y, col), True))
        else:
            self.ways += [((row - 2, col), y > 0), ((row + 2, col), y < plan.ys - 1)]
        self.ways += [((row, col - 2), z > 0), ((row, col + 2), z < plan.zs - 1)]

    def greet(self):
        plan, barrier = self.plan, pltpu.get_barrier_semaphore()
        count = 1
        pl.semaphore_signal(barrier, inc=1, device_id=self.partner, device_id_type=MESH)
        for target, there in self.ways:
            if there is True:
                count += 1
                pl.semaphore_signal(barrier, inc=1, device_id=target, device_id_type=MESH)
            else:
                count += there.astype(jnp.int32)

                @pl.when(there)
                def _():
                    pl.semaphore_signal(barrier, inc=1, device_id=target, device_id_type=MESH)
        if plan.split and plan.ys > 2:
            count += plan.ys - 1
            for far in range(1, plan.ys):
                target = (2 * lax.rem(plan.y + far, plan.ys) + plan.core, plan.col)
                pl.semaphore_signal(barrier, inc=1, device_id=target, device_id_type=MESH)
        pl.semaphore_wait(barrier, count)

    def own(self, piece, extra=False):
        plan = self.plan
        if extra:
            start = lax.rem(plan.col, plan.q) * plan.w + (piece - plan.pieces) * plan.ph
            offset = plan.pw
        else:
            start, offset = piece * plan.ph, plan.offset(plan.row, plan.col, piece)
        return self.x_ref.at[pl.ds(pl.multiple_of(start, plan.ph), plan.ph), pl.ds(offset, plan.pw)]

    def link(self, act, way, src, sy, sc, piece):
        dst, at = self.stage.at[sy, sc, piece], sy * self.plan.col_n + sc
        getattr(pltpu.make_async_remote_copy(
            src_ref=dst if src is None else src, dst_ref=dst, send_sem=self.send.at[way, at, piece],
            recv_sem=self.recv.at[at, piece], device_id=self.ways[way][0], device_id_type=MESH), act)()

    def across(self, act, src, sy, sc, piece):
        plan, at = self.plan, sy * self.plan.col_n + sc
        if not plan.halved:
            return

        @pl.when((piece < plan.pieces) & jnp.logical_not(plan.is_mine(sc)))
        def _():
            getattr(pltpu.make_async_remote_copy(
                src_ref=self.stage.at[sy, sc, piece] if src is None else src, dst_ref=self.cross.at[sy, sc, piece],
                send_sem=self.cross_send.at[at, piece], recv_sem=self.cross_recv.at[at, piece],
                device_id=self.partner, device_id_type=MESH), act)()

    def onward(self, act, src, where, piece, spot):
        plan = self.plan
        dx, dy, y_sign, z_sign = where
        sy, sc, dz, _ = spot
        z_last = piece < plan.pieces // 4
        y_first = lax.rem(piece, 2) == 1
        near = dz == 0
        z_done = jnp.logical_or(jnp.logical_not(z_last), near)

        def go(way, when):
            there = self.ways[way][1]

            @pl.when(when if there is True else when & there)
            def _():
                self.link(act, way, src, sy, sc, piece)

        first = len(self.ways) - 2
        for way, sign in ((first, 1), (first + 1, -1)):
            here = near | (z_sign == sign)
            go(way, here if dx == 0 and dy == 0 else here & z_last)
        if dx == 0:
            go(0, z_done if dy == 0 else z_done & y_first)
        y_open = z_done if dx == 0 else z_done & jnp.logical_not(y_first)
        if plan.ys == 2:
            if dy == 0:
                go(1, y_open)
        else:
            for way, sign in ((1, 1), (2, -1)):
                if dy == 0 or y_sign == sign:
                    go(way, y_open)

    def spot(self, where, far, piece):
        plan = self.plan
        dx, dy, y_sign, z_sign = where
        dz = far - dx - dy
        sz = plan.z + z_sign * dz
        sy = 1 - plan.y if plan.ys == 2 and dy else plan.y + y_sign * dy
        sc = 2 * sz + (1 - plan.x if dx else plan.x)
        there = (dz >= (0 if z_sign > 0 else 1)) & (sz >= 0) & (sz < plan.zs)
        if plan.ys != 2:
            there = there & (sy >= 0) & (sy < plan.ys)
        if plan.extra:
            there = there & ((piece < plan.pieces) | plan.is_diagonal(sy, sc))
        return sy, sc, dz, there

    def begin(self):
        plan = self.plan
        here = (0, 0, 0, 1)

        def step(extra):
            def start(piece, carry):
                src = self.own(piece, extra)
                self.onward("start", src, here, piece, (plan.y, plan.col, jnp.int32(0), None))
                self.across("start", src, plan.y, plan.col, piece)
                return carry
            return start
        lax.fori_loop(0, plan.pieces, step(False), 0)
        if plan.extra:
            @pl.when(plan.is_diagonal(plan.y, plan.col))
            def _():
                lax.fori_loop(plan.pieces, plan.total, step(True), 0)

    def wait_arrival(self, sy, sc, piece):
        dst = self.stage.at[sy, sc, piece]
        pltpu.make_async_remote_copy(
            src_ref=dst, dst_ref=dst, send_sem=self.send.at[0, 0, 0], recv_sem=self.recv.at[sy * self.plan.col_n + sc, piece],
            device_id=self.ways[0][0], device_id_type=MESH).wait_recv()

    def wait_cross(self, sy, sc, piece):
        dst = self.cross.at[sy, sc, piece]
        pltpu.make_async_remote_copy(
            src_ref=dst, dst_ref=dst, send_sem=self.cross_send.at[0, 0],
            recv_sem=self.cross_recv.at[sy * self.plan.col_n + sc, piece],
            device_id=self.partner, device_id_type=MESH).wait_recv()

    def lay(self, tile, sy, sc, piece):
        plan = self.plan
        h, w, q, ph, pw = plan.h, plan.w, plan.q, plan.ph, plan.pw
        inner = lax.rem(sc, q) * w
        row, col = piece * ph, inner + plan.offset(2 * sy + plan.core, sc, piece)
        if plan.extra:
            normal, past = piece < plan.pieces, (piece - plan.pieces) * ph
            row, col = jnp.where(normal, row, inner + past), jnp.where(normal, col, inner + pw)
        base = plan.place(sc // q)
        self.put(tile[...], sy * h + row, base + col)
        if plan.halved:
            block = ((2 * sy + plan.core) * h + row) // w

            @pl.when((plan.is_mine(sc) & (block != sc)) | jnp.logical_not(normal))
            def _():
                self.put(tile[...].T, (sc // q // 2) * h + col, sy * h + row)

    def lay_turned(self, tile, sy, sc, piece):
        plan = self.plan
        source = 2 * sy + 1 - plan.core
        at = (sc // plan.q // 2) * plan.h + lax.rem(sc, plan.q) * plan.w + plan.offset(source, sc, piece)
        self.put(tile[...].T, at, plan.place(source) + piece * plan.ph)

    def run(self):
        plan = self.plan
        wheres = places(plan)

        def fetch(act, src, slot, e):
            getattr(pltpu.make_async_copy(src, self.tiles.at[slot, e], self.tile_sem.at[slot, e]), act)()

        def fetch_turned(act, sy, sc, piece, slot, e):
            getattr(pltpu.make_async_copy(
                self.cross.at[sy, sc, piece], self.turned.at[slot, e], self.turned_sem.at[slot, e]), act)()

        def turn(where, far, piece):
            sy, sc, dz, there = self.spot(where, far, piece)
            return sy, sc, there & (piece < plan.pieces) & plan.is_mine(sc)

        def one(far, piece, e, where):
            slot = lax.rem(far * plan.total + piece, 2)
            spot = self.spot(where, far, piece)
            sy, sc, _, there = spot

            @pl.when(there & (far > 0))
            def _():
                self.wait_arrival(sy, sc, piece)
                self.onward("start", None, where, piece, spot)
                self.across("start", None, sy, sc, piece)

            wrap = (piece == 0).astype(jnp.int32)
            old_far, old_piece = far - wrap, piece - 1 + wrap * plan.total
            oy, oc, _, old = self.spot(where, old_far, old_piece)

            @pl.when(old)
            def _():
                fetch("wait", self.stage.at[oy, oc, old_piece], 1 - slot, e)
                self.lay(self.tiles.at[1 - slot, e], oy, oc, old_piece)

            @pl.when(there & (far > 0))
            def _():
                fetch("start", self.stage.at[sy, sc, piece], slot, e)
            if where == (0, 0, 0, 1):
                @pl.when(there & (far == 0) & (piece < plan.pieces))
                def _():
                    fetch("start", self.own(piece), slot, e)
                if plan.extra:
                    @pl.when(there & (far == 0) & (piece >= plan.pieces))
                    def _():
                        fetch("start", self.own(piece, True), slot, e)

            if plan.halved:
                ty, tc, old_turn = turn(where, old_far - 1, old_piece)

                @pl.when(old_turn)
                def _():
                    fetch_turned("wait", ty, tc, old_piece, 1 - slot, e)
                    self.lay_turned(self.turned.at[1 - slot, e], ty, tc, old_piece)
                uy, uc, new_turn = turn(where, far - 1, piece)

                @pl.when(new_turn)
                def _():
                    self.wait_cross(uy, uc, piece)
                    fetch_turned("start", uy, uc, piece, slot, e)
                vy, vc, _, sent = self.spot(where, far - 1, piece)

                @pl.when(sent)
                def _():
                    self.across("wait_send", None, vy, vc, piece)
            done = self.spot(where, far - 2, piece)

            @pl.when(done[3])
            def _():
                self.onward("wait_send", None, where, piece, done)

        def round_(far, carry):
            def step(piece, carry):
                for e, where in enumerate(wheres):
                    one(far, piece, e, where)
                return carry
            return lax.fori_loop(0, plan.total, step, carry)

        lax.fori_loop(0, plan.zs + plan.ys + 1, round_, 0)


STEPS = 8


def weights(step):
    def pick(table, other):
        value = jnp.float32(other)
        for at, entry in table:
            value = jnp.where(step == at, jnp.float32(entry), value)
        return value
    return pick(((1, 1.5),), 0.0), pick(((4, 1.5),), 0.0), pick(((1, -0.5), (4, -0.5)), 1.0)


def sign_kernel(plan, x_ref, *rest):
    if plan.halved:
        out, stage, cross = rest[:3]
        rest = rest[3:]
    else:
        out, stage = rest[:2]
        cross, rest = None, rest[2:]
    (high, low, own_high, own_low, peer_high, peer_low, panel, peer, first, second, tiles, turned, squares, peer_squares,
     scale, recv, send_sem, cross_recv, cross_send, tile_sem, turned_sem, panel_send, panel_recv, square_sems, out_local,
     out_send, out_recv) = rest
    plan.locate()
    col, core, y = plan.col, plan.core, plan.y
    h, w, q, half, cw = plan.h, plan.w, plan.q, plan.n // 2, plan.cw

    def put(tile, at, to):
        top = tile.astype(BF16)
        rest = (tile - top.astype(F32)).astype(BF16)
        rows = pl.ds(pl.multiple_of(at, tile.shape[0]), tile.shape[0])
        cols = pl.ds(pl.multiple_of(to, tile.shape[1]), tile.shape[1])
        high[rows, cols] = top
        low[rows, cols] = rest
        both = tile * tile
        squares[...] += jnp.sum(both.reshape(tile.shape[0] // 8, 8, tile.shape[1] // 128, 128), axis=(0, 2))

    gather = Gather(plan, x_ref, stage, cross, put, tiles, turned,
                    (recv, send_sem, cross_recv, cross_send, tile_sem, turned_sem))
    gather.greet()
    gather.begin()
    squares[...] = jnp.zeros_like(squares)
    gather.run()
    partner = gather.partner

    share = pltpu.make_async_remote_copy(src_ref=squares, dst_ref=peer_squares, send_sem=square_sems.at[0],
                                         recv_sem=square_sems.at[1], device_id=partner, device_id_type=MESH)
    share.start()
    share.wait()
    total = jnp.sum(jnp.sum(squares[...] + peer_squares[...], axis=0, keepdims=True), axis=1, keepdims=True)
    scale[...] = jnp.broadcast_to(jnp.sqrt(plan.n / total), scale.shape)

    def rows_of(tile):
        return pl.ds(pl.multiple_of(tile * h, h), h)

    def send(slot, tile):
        rows = rows_of(tile)
        return pltpu.make_async_remote_copy(
            src_ref=panel.at[slot, rows], dst_ref=peer.at[slot, rows], send_sem=panel_send.at[slot, tile],
            recv_sem=panel_recv.at[slot, tile], device_id=partner, device_id_type=MESH)

    def parts(value):
        top = value.astype(BF16)
        return top, (value - top.astype(F32)).astype(BF16)

    start = plan.place(col // q) + lax.rem(col, q) * w + (y * cw if plan.split else 0)
    mine_cols = pl.ds(pl.multiple_of(start, cw), cw)

    def begin(tile, carry):
        rows = rows_of(tile)
        value = scale[0:1, 0:1] * (high[rows, mine_cols].astype(F32) + low[rows, mine_cols].astype(F32))
        first[rows, :] = value
        second[rows, :] = value
        panel[0, rows] = value
        own_high[rows, :], own_low[rows, :] = parts(value)
        send(0, tile).start()
        return carry
    lax.fori_loop(0, plan.ys, begin, 0)

    def product(rows, cols, b_high, b_low):
        a_high, a_low = high[rows, cols], low[rows, cols]
        top = b_high[...]
        acc = jnp.dot(a_high, top, preferred_element_type=F32)
        acc += jnp.dot(a_high, b_low[...], preferred_element_type=F32)
        return acc + jnp.dot(a_low, top, preferred_element_type=F32)

    def near(slot, tile):
        rows = rows_of(tile)
        panel[slot, rows] = product(rows, slice(0, half), own_high, own_low)

    def far(slot, rows):
        return scale[0:1, 0:1] * (panel[slot, rows] + product(rows, slice(half, 2 * half), peer_high, peer_low))

    def meet(slot):
        for tile in range(plan.ys):
            send(slot, tile).wait_recv()
        peer_high[...], peer_low[...] = parts(peer[slot])

    def sent(slot):
        for tile in range(plan.ys):
            send(slot, tile).wait_send()

    def step_(step, carry):
        now, later = lax.rem(step, 2), lax.rem(step + 1, 2)

        @pl.when(step > 0)
        def _():
            sent(later)

        def near_(tile, carry):
            near(later, tile)
            return carry
        lax.fori_loop(0, plan.ys, near_, 0)
        meet(now)
        a, b, c = weights(step)

        def far_(tile, carry):
            rows = rows_of(tile)
            value = a * first[rows, :] + b * second[rows, :] + c * far(later, rows)
            panel[later, rows] = value
            own_high[rows, :], own_low[rows, :] = parts(value)
            send(later, tile).start()

            @pl.when(step == 1)
            def _():
                first[rows, :] = value

            @pl.when((step == 2) | (step == 5))
            def _():
                second[rows, :] = value
            return carry
        lax.fori_loop(0, plan.ys, far_, 0)
        return carry
    lax.fori_loop(0, STEPS - 1, step_, 0)

    now, later = (STEPS - 1) % 2, STEPS % 2
    chunk = h // CHUNKS
    sent(later)

    def deliver(tile, far, part):
        return pltpu.make_async_remote_copy(
            src_ref=panel.at[later, pl.ds(pl.multiple_of(tile * h + part * chunk, chunk), chunk)],
            dst_ref=out.at[pl.ds(pl.multiple_of(part * chunk, chunk), chunk), pl.ds(pl.multiple_of(y * cw, cw), cw)],
            send_sem=out_send.at[far, part], recv_sem=out_recv.at[far, part],
            device_id=(2 * tile + core, col), device_id_type=MESH)

    def result(far_off, carry):
        tile = lax.rem(y + 1 + far_off, plan.ys)
        near(later, tile)

        @pl.when(far_off == 0)
        def _():
            meet(now)

        def piece(part, carry):
            rows = pl.ds(pl.multiple_of(tile * h + part * chunk, chunk), chunk)
            panel[later, rows] = 1.5 * first[rows, :] - 0.75 * second[rows, :] + 0.25 * far(later, rows)
            if plan.split:
                @pl.when(far_off < plan.ys - 1)
                def _():
                    deliver(tile, far_off, part).start()
            return carry
        lax.fori_loop(0, CHUNKS, piece, 0)
        return carry
    lax.fori_loop(0, plan.ys, result, 0)

    local = pltpu.make_async_copy(
        panel.at[later, rows_of(y)],
        out.at[:, pl.ds(pl.multiple_of(y * cw if plan.split else 0, cw), cw)], out_local)
    local.start()
    sent(now)
    if plan.split:
        for far_off in range(plan.ys - 1):
            for part in range(CHUNKS):
                deliver(lax.rem(y + 1 + far_off, plan.ys), far_off, part).wait()
    local.wait()


CHUNKS = 2


def shards(row_n, col_n, matrix):
    plan = Plan(row_n, col_n, matrix.shape)
    h, half, cw = plan.h, plan.n // 2, plan.cw
    vmem = pltpu.VMEM
    full, count = (plan.ys, plan.col_n), plan.ys * plan.col_n
    shapes = [jax.ShapeDtypeStruct((h, plan.w), F32),
              jax.ShapeDtypeStruct((*full, plan.total, plan.ph, plan.pw), F32)]
    if plan.halved:
        shapes.append(jax.ShapeDtypeStruct((*full, plan.pieces, plan.ph, plan.pw), F32))
    spots = len(places(plan))
    turned = (2, spots, plan.ph, plan.pw) if plan.halved else (8, 128)
    return pl.pallas_call(
        functools.partial(sign_kernel, plan),
        out_shape=shapes, in_specs=[ANY], out_specs=[ANY] * len(shapes),
        scratch_shapes=[vmem((half, plan.n), BF16)] * 2 + [vmem((half, cw), BF16)] * 4
        + [vmem((2, half, cw), F32)] * 2 + [vmem((half, cw), F32)] * 2
        + [vmem((2, spots, plan.ph, plan.pw), F32), vmem(turned, F32)] + [vmem((8, 128), F32)] * 3
        + [DMA((count, plan.total)), DMA((4 if plan.ys == 2 else 5, count, plan.total)), DMA((count, plan.pieces)),
           DMA((count, plan.pieces)), DMA((2, spots)), DMA((2, spots))]
        + [DMA((2, plan.ys)), DMA((2, plan.ys)), DMA((2,)), DMA(()), DMA((plan.ys - 1, CHUNKS)),
           DMA((plan.ys - 1, CHUNKS))],
        compiler_params=pltpu.CompilerParams(collective_id=0, has_side_effects=True, vmem_limit_bytes=63 * 2**20),
        name="sign",
    )(matrix)[0]


def solution(mesh):
    body = functools.partial(shards, mesh.shape["row"], mesh.shape["col"])
    return jax.shard_map(body, mesh=mesh, in_specs=(P("row", "col"),), out_specs=P("row", "col"), check_vma=False)
```

```python
import functools

import jax
import jax.numpy as jnp
from jax import lax
from jax.experimental import pallas as pl
from jax.experimental.pallas import tpu as pltpu
from jax.sharding import PartitionSpec as P

ITERS = 2
MESH = pl.DeviceIdType.MESH
ANY = pl.BlockSpec(memory_space=pl.ANY)
DMA = pltpu.SemaphoreType.DMA
F32, BF16 = jnp.float32, jnp.bfloat16


class Plan:
    def __init__(self, row_n, col_n, block):
        self.row_n, self.col_n = row_n, col_n
        self.h, self.w = block
        self.n = self.h * row_n
        self.ys, self.zs = row_n // 2, col_n // 2
        self.q = self.h // self.w
        self.halved = self.w % 256 == 0
        self.pw = self.w // 2 if self.halved else self.w
        self.pieces = max(2, self.h * self.pw // 32768)
        self.ph = self.h // self.pieces
        self.extra = self.pw // self.ph if self.halved else 0
        self.total = self.pieces + self.extra
        self.split = (self.w // self.ys) % 128 == 0
        self.cw = self.w // self.ys if self.split else self.w
        self.bulk = self.ys == 2 and self.q % 2 == 0

    def locate(self):
        self.row, self.col = lax.axis_index("row"), lax.axis_index("col")
        self.core, self.y = lax.rem(self.row, 2), self.row // 2
        self.x, self.z = lax.rem(self.col, 2), self.col // 2

    def offset(self, row, col, piece):
        if not self.halved:
            return 0
        start = piece * self.ph
        upper = ((row * self.h + start) // self.w < col).astype(jnp.int32)
        return pl.multiple_of(self.pw * lax.rem(start // self.pw + upper, 2), self.pw)

    def place(self, row_block):
        swap = lax.rem(lax.rem(row_block, 2) + self.core, 2)
        return (swap * self.ys + row_block // 2) * self.h

    def is_mine(self, col):
        return lax.rem(col // self.q, 2) == self.core

    def is_diagonal(self, y, col):
        return col // self.q == 2 * y + self.core


def places(plan):
    ys = ((0, 0), (1, 0)) if plan.ys == 2 else ((0, 0),) + tuple(
        (far, sign) for far in range(1, plan.ys) for sign in (1, -1))
    return [(dx, dy, y_sign, z_sign) for dx in (0, 1) for dy, y_sign in ys for z_sign in (1, -1)]


class Gather:
    def __init__(self, plan, x_ref, stage, cross, put, tiles, turned, sems):
        self.plan, self.x_ref, self.stage, self.cross, self.put = plan, x_ref, stage, cross, put
        self.tiles, self.turned = tiles, turned
        self.recv, self.send, self.cross_recv, self.cross_send, self.tile_sem, self.turned_sem = sems
        row, col, x, y, z = plan.row, plan.col, plan.x, plan.y, plan.z
        self.partner = (row + 1 - 2 * plan.core, col)
        self.ways = [((row, col + 1 - 2 * x), True)]
        if plan.ys == 2:
            self.ways.append(((row + 2 - 4 * y, col), True))
        else:
            self.ways += [((row - 2, col), y > 0), ((row + 2, col), y < plan.ys - 1)]
        self.ways += [((row, col - 2), z > 0), ((row, col + 2), z < plan.zs - 1)]

    def greet(self):
        plan, barrier = self.plan, pltpu.get_barrier_semaphore()
        count = 1
        pl.semaphore_signal(barrier, inc=1, device_id=self.partner, device_id_type=MESH)
        for target, there in self.ways:
            if there is True:
                count += 1
                pl.semaphore_signal(barrier, inc=1, device_id=target, device_id_type=MESH)
            else:
                count += there.astype(jnp.int32)

                @pl.when(there)
                def _():
                    pl.semaphore_signal(barrier, inc=1, device_id=target, device_id_type=MESH)
        if plan.split and plan.ys > 2:
            count += plan.ys - 1
            for far in range(1, plan.ys):
                target = (2 * lax.rem(plan.y + far, plan.ys) + plan.core, plan.col)
                pl.semaphore_signal(barrier, inc=1, device_id=target, device_id_type=MESH)
        pl.semaphore_wait(barrier, count)

    def own(self, piece, extra=False):
        plan = self.plan
        if extra:
            start = lax.rem(plan.col, plan.q) * plan.w + (piece - plan.pieces) * plan.ph
            offset = plan.pw
        else:
            start, offset = piece * plan.ph, plan.offset(plan.row, plan.col, piece)
        return self.x_ref.at[pl.ds(pl.multiple_of(start, plan.ph), plan.ph), pl.ds(offset, plan.pw)]

    def held(self, sy, sc, piece):
        return self.stage.at[(sy * self.plan.col_n + sc) * self.plan.total + piece]

    def crossed(self, sy, sc, piece):
        return self.cross.at[(sy * self.plan.col_n + sc) * self.plan.pieces + piece]

    def link(self, act, way, src, sy, sc, piece):
        dst, at = self.held(sy, sc, piece), sy * self.plan.col_n + sc
        getattr(pltpu.make_async_remote_copy(
            src_ref=dst if src is None else src, dst_ref=dst,
            send_sem=self.send.at[way] if self.plan.bulk else self.send.at[way, at, piece],
            recv_sem=self.recv.at[at, piece], device_id=self.ways[way][0], device_id_type=MESH), act)()

    def across(self, src, sy, sc, piece):
        plan = self.plan
        if not plan.halved:
            return

        @pl.when((piece < plan.pieces) & jnp.logical_not(plan.is_mine(sc)))
        def _():
            pltpu.make_async_remote_copy(
                src_ref=self.held(sy, sc, piece) if src is None else src, dst_ref=self.crossed(sy, sc, piece),
                send_sem=self.cross_send, recv_sem=self.cross_recv.at[sy * plan.col_n + sc, piece],
                device_id=self.partner, device_id_type=MESH).start()

    def onward(self, act, src, where, piece, spot):
        plan = self.plan
        dx, dy, y_sign, z_sign = where
        sy, sc, dz = spot[:3]
        z_last = piece < plan.pieces // 4
        y_first = lax.rem(piece, 2) == 1
        near = dz == 0
        z_done = jnp.logical_or(jnp.logical_not(z_last), near)

        def go(way, when):
            there = self.ways[way][1]

            @pl.when(when if there is True else when & there)
            def _():
                self.link(act, way, src, sy, sc, piece)

        first = len(self.ways) - 2
        for way, sign in ((first, 1), (first + 1, -1)):
            here = near | (z_sign == sign)
            go(way, here if dx == 0 and dy == 0 else here & z_last)
        if dx == 0:
            go(0, z_done if dy == 0 else z_done & y_first)
        y_open = z_done if dx == 0 else z_done & jnp.logical_not(y_first)
        if plan.ys == 2:
            if dy == 0:
                go(1, y_open)
        else:
            for way, sign in ((1, 1), (2, -1)):
                if dy == 0 or y_sign == sign:
                    go(way, y_open)

    def spot(self, where, far):
        plan = self.plan
        dx, dy, y_sign, z_sign = where
        dz = far - dx - dy
        sz = plan.z + z_sign * dz
        sy = 1 - plan.y if plan.ys == 2 and dy else plan.y + y_sign * dy
        sc = 2 * sz + (1 - plan.x if dx else plan.x)
        there = (dz >= (0 if z_sign > 0 else 1)) & (sz >= 0) & (sz < plan.zs)
        if plan.ys != 2:
            there = there & (sy >= 0) & (sy < plan.ys)
        return sy, sc, dz, there, plan.is_diagonal(sy, sc) if plan.extra else None

    def has(self, spot, piece):
        there = spot[3] & (piece >= 0)
        if self.plan.extra:
            return there & ((piece < self.plan.pieces) | (spot[4] & (piece < self.plan.total)))
        return there & (piece < self.plan.total)

    def begin(self):
        plan = self.plan
        here = (0, 0, 0, 1)

        def step(extra):
            def start(piece, carry):
                src = self.own(piece, extra)
                self.onward("start", src, here, piece, (plan.y, plan.col, jnp.int32(0)))
                self.across(src, plan.y, plan.col, piece)
                return carry
            return start
        lax.fori_loop(0, plan.pieces, step(False), 0)
        if plan.extra:
            @pl.when(plan.is_diagonal(plan.y, plan.col))
            def _():
                lax.fori_loop(plan.pieces, plan.total, step(True), 0)

    def wait_arrival(self, sy, sc, piece):
        dst = self.held(sy, sc, piece)
        pltpu.make_async_remote_copy(
            src_ref=dst, dst_ref=dst, send_sem=self.send.at[0] if self.plan.bulk else self.send.at[0, 0, 0], recv_sem=self.recv.at[sy * self.plan.col_n + sc, piece],
            device_id=self.ways[0][0], device_id_type=MESH).wait_recv()

    def wait_cross(self, sy, sc, piece):
        dst = self.crossed(sy, sc, piece)
        pltpu.make_async_remote_copy(
            src_ref=dst, dst_ref=dst, send_sem=self.cross_send,
            recv_sem=self.cross_recv.at[sy * self.plan.col_n + sc, piece],
            device_id=self.partner, device_id_type=MESH).wait_recv()

    def lay(self, tile, sy, sc, piece):
        plan = self.plan
        h, w, q, ph, pw = plan.h, plan.w, plan.q, plan.ph, plan.pw
        inner = lax.rem(sc, q) * w
        row, col = piece * ph, inner + plan.offset(2 * sy + plan.core, sc, piece)
        if plan.extra:
            normal, past = piece < plan.pieces, (piece - plan.pieces) * ph
            row, col = jnp.where(normal, row, inner + past), jnp.where(normal, col, inner + pw)
        base = plan.place(sc // q)
        self.put(tile[...], sy * h + row, base + col)
        if plan.halved:
            block = ((2 * sy + plan.core) * h + row) // w

            @pl.when((plan.is_mine(sc) & (block != sc)) | jnp.logical_not(normal))
            def _():
                self.put(tile[...].T, (sc // q // 2) * h + col, sy * h + row)

    def lay_turned(self, tile, sy, sc, piece):
        plan = self.plan
        source = 2 * sy + 1 - plan.core
        at = (sc // plan.q // 2) * plan.h + lax.rem(sc, plan.q) * plan.w + plan.offset(source, sc, piece)
        self.put(tile[...].T, at, plan.place(source) + piece * plan.ph)

    def run(self):
        plan = self.plan
        wheres = places(plan)

        def fetch(act, src, slot, e):
            getattr(pltpu.make_async_copy(src, self.tiles.at[slot, e], self.tile_sem.at[slot, e]), act)()

        def fetch_turned(act, sy, sc, piece, slot, e):
            getattr(pltpu.make_async_copy(
                self.crossed(sy, sc, piece), self.turned.at[slot, e], self.turned_sem.at[slot, e]), act)()

        def arriving(far, piece, slot, e, where, spot):
            sy, sc = spot[:2]

            @pl.when(self.has(spot, piece) & (far > 0))
            def _():
                self.wait_arrival(sy, sc, piece)
                self.onward("start", None, where, piece, spot)
                self.across(None, sy, sc, piece)

            @pl.when(self.has(spot, piece - 1))
            def _():
                fetch("wait", self.held(sy, sc, piece - 1), 1 - slot, e)
                self.lay(self.tiles.at[1 - slot, e], sy, sc, piece - 1)

            @pl.when(self.has(spot, piece) & (far > 0))
            def _():
                fetch("start", self.held(sy, sc, piece), slot, e)
            if where == (0, 0, 0, 1):
                @pl.when(self.has(spot, piece) & (far == 0) & (piece < plan.pieces))
                def _():
                    fetch("start", self.own(piece), slot, e)
                if plan.extra:
                    @pl.when(self.has(spot, piece) & (far == 0) & (piece >= plan.pieces))
                    def _():
                        fetch("start", self.own(piece, True), slot, e)

        def crossing(piece, slot, e, spot):
            sy, sc = spot[:2]

            @pl.when((piece > 0) & (piece <= plan.pieces))
            def _():
                fetch_turned("wait", sy, sc, piece - 1, 1 - slot, e)
                self.lay_turned(self.turned.at[1 - slot, e], sy, sc, piece - 1)

            @pl.when(piece < plan.pieces)
            def _():
                self.wait_cross(sy, sc, piece)
                fetch_turned("start", sy, sc, piece, slot, e)

        def round_(far, carry):
            now = [self.spot(where, far) for where in wheres]
            before = [self.spot(where, far - 1) for where in wheres]

            def step(piece, carry):
                slot = lax.rem(piece, 2)
                for e, where in enumerate(wheres):
                    @pl.when(now[e][3])
                    def _():
                        arriving(far, piece, slot, e, where, now[e])
                    if plan.halved:
                        @pl.when(before[e][3] & plan.is_mine(before[e][1]))
                        def _():
                            crossing(piece, slot, e, before[e])
                return carry
            return lax.fori_loop(0, plan.total + 1, step, carry)

        lax.fori_loop(0, plan.zs + plan.ys + 1, round_, 0)

    def finish(self):
        plan = self.plan
        if plan.halved:
            some = self.cross.at[pl.ds(0, plan.ys * plan.col_n // 2 * plan.pieces)]
            pltpu.make_async_remote_copy(
                src_ref=some, dst_ref=some, send_sem=self.cross_send, recv_sem=self.cross_recv.at[0, 0],
                device_id=self.partner, device_id_type=MESH).wait_send()
        if not plan.bulk:
            def step(far, carry):
                def one(piece, carry):
                    for where in places(plan):
                        spot = self.spot(where, far)

                        @pl.when(self.has(spot, piece))
                        def _():
                            self.onward("wait_send", None, where, piece, spot)
                    return carry
                return lax.fori_loop(0, plan.total, one, carry)
            lax.fori_loop(0, plan.zs + plan.ys, step, 0)
            return

        def settle(way, count):
            some = self.stage.at[pl.ds(0, count)]
            pltpu.make_async_remote_copy(
                src_ref=some, dst_ref=some, send_sem=self.send.at[way], recv_sem=self.recv.at[0, 0],
                device_id=self.ways[way][0], device_id_type=MESH).wait_send()

        zs, last, m = plan.zs, plan.pieces // 4, plan.q // 2
        even_last, odd_last = (last + 1) // 2, last // 2
        even = (plan.pieces + 1) // 2 - even_last
        odd = plan.pieces // 2 - odd_last
        more = range(plan.pieces, plan.total)
        even_more = sum(p % 2 == 0 for p in more)
        odd_more = plan.extra - even_more
        settle(0, zs * (even + 2 * odd) + even_last + 2 * odd_last + m * (even_more + 2 * odd_more))
        settle(1, zs * (2 * even + odd) + 2 * even_last + odd_last + m * (2 * even_more + odd_more))
        each = even + odd + 4 * last
        for way, sign in ((2, 1), (3, -1)):
            marked = sum(
                ((sign * (sz - plan.z) >= 0) & (sz // m == 2 * plan.y + plan.core)).astype(jnp.int32) for sz in range(zs))
            for at in range(zs):
                spots = zs - at if sign > 0 else at + 1
                if at == (0 if sign > 0 else zs - 1):
                    continue
                for extras in range(m + 1 if plan.extra else 1):
                    @pl.when((plan.z == at) & (marked == extras if plan.extra else True))
                    def _():
                        settle(way, spots * each + extras * plan.extra)


STEPS = 8


def weights(step):
    def pick(table, other):
        value = jnp.float32(other)
        for at, entry in table:
            value = jnp.where(step == at, jnp.float32(entry), value)
        return value
    return pick(((1, 1.5),), 0.0), pick(((4, 1.5),), 0.0), pick(((1, -0.5), (4, -0.5)), 1.0)


def sign_kernel(plan, x_ref, *rest):
    if plan.halved:
        out, stage, cross = rest[:3]
        rest = rest[3:]
    else:
        out, stage = rest[:2]
        cross, rest = None, rest[2:]
    (high, low, own_high, own_low, peer_high, peer_low, panel, peer, first, second, tiles, turned, squares, peer_squares,
     scale, recv, send_sem, cross_recv, cross_send, tile_sem, turned_sem, panel_send, panel_recv, square_sems, out_local,
     out_send, out_recv) = rest
    plan.locate()
    col, core, y = plan.col, plan.core, plan.y
    h, w, q, half, cw = plan.h, plan.w, plan.q, plan.n // 2, plan.cw

    def put(tile, at, to):
        top = tile.astype(BF16)
        rest = (tile - top.astype(F32)).astype(BF16)
        rows = pl.ds(pl.multiple_of(at, tile.shape[0]), tile.shape[0])
        cols = pl.ds(pl.multiple_of(to, tile.shape[1]), tile.shape[1])
        high[rows, cols] = top
        low[rows, cols] = rest
        both = tile * tile
        squares[...] += jnp.sum(both.reshape(tile.shape[0] // 8, 8, tile.shape[1] // 128, 128), axis=(0, 2))

    gather = Gather(plan, x_ref, stage, cross, put, tiles, turned,
                    (recv, send_sem, cross_recv, cross_send, tile_sem, turned_sem))
    gather.greet()
    gather.begin()
    squares[...] = jnp.zeros_like(squares)
    gather.run()
    partner = gather.partner

    share = pltpu.make_async_remote_copy(src_ref=squares, dst_ref=peer_squares, send_sem=square_sems.at[0],
                                         recv_sem=square_sems.at[1], device_id=partner, device_id_type=MESH)
    share.start()
    share.wait()
    total = jnp.sum(jnp.sum(squares[...] + peer_squares[...], axis=0, keepdims=True), axis=1, keepdims=True)
    scale[...] = jnp.broadcast_to(jnp.sqrt(plan.n / total), scale.shape)

    def rows_of(tile):
        return pl.ds(pl.multiple_of(tile * h, h), h)

    def send(slot, tile):
        rows = rows_of(tile)
        return pltpu.make_async_remote_copy(
            src_ref=panel.at[slot, rows], dst_ref=peer.at[slot, rows], send_sem=panel_send.at[slot, tile],
            recv_sem=panel_recv.at[slot, tile], device_id=partner, device_id_type=MESH)

    def parts(value):
        top = value.astype(BF16)
        return top, (value - top.astype(F32)).astype(BF16)

    start = plan.place(col // q) + lax.rem(col, q) * w + (y * cw if plan.split else 0)
    mine_cols = pl.ds(pl.multiple_of(start, cw), cw)

    def begin(tile, carry):
        rows = rows_of(tile)
        value = scale[0:1, 0:1] * (high[rows, mine_cols].astype(F32) + low[rows, mine_cols].astype(F32))
        first[rows, :] = value
        second[rows, :] = value
        panel[0, rows] = value
        own_high[rows, :], own_low[rows, :] = parts(value)
        send(0, tile).start()
        return carry
    lax.fori_loop(0, plan.ys, begin, 0)

    def product(rows, cols, b_high, b_low):
        a_high, a_low = high[rows, cols], low[rows, cols]
        top = b_high[...]
        acc = jnp.dot(a_high, top, preferred_element_type=F32)
        acc += jnp.dot(a_high, b_low[...], preferred_element_type=F32)
        return acc + jnp.dot(a_low, top, preferred_element_type=F32)

    def near(slot, tile):
        rows = rows_of(tile)
        panel[slot, rows] = product(rows, slice(0, half), own_high, own_low)

    def far(slot, rows):
        return scale[0:1, 0:1] * (panel[slot, rows] + product(rows, slice(half, 2 * half), peer_high, peer_low))

    def meet(slot):
        for tile in range(plan.ys):
            send(slot, tile).wait_recv()
        peer_high[...], peer_low[...] = parts(peer[slot])

    def sent(slot):
        for tile in range(plan.ys):
            send(slot, tile).wait_send()

    def step_(step, carry):
        now, later = lax.rem(step, 2), lax.rem(step + 1, 2)

        @pl.when(step > 0)
        def _():
            sent(later)

        def near_(tile, carry):
            near(later, tile)
            return carry
        lax.fori_loop(0, plan.ys, near_, 0)
        meet(now)
        a, b, c = weights(step)

        def far_(tile, carry):
            rows = rows_of(tile)
            value = a * first[rows, :] + b * second[rows, :] + c * far(later, rows)
            panel[later, rows] = value
            own_high[rows, :], own_low[rows, :] = parts(value)
            send(later, tile).start()

            @pl.when(step == 1)
            def _():
                first[rows, :] = value

            @pl.when((step == 2) | (step == 5))
            def _():
                second[rows, :] = value
            return carry
        lax.fori_loop(0, plan.ys, far_, 0)
        return carry
    lax.fori_loop(0, STEPS - 1, step_, 0)

    now, later = (STEPS - 1) % 2, STEPS % 2
    chunk = h // CHUNKS
    sent(later)

    def deliver(tile, far, part):
        return pltpu.make_async_remote_copy(
            src_ref=panel.at[later, pl.ds(pl.multiple_of(tile * h + part * chunk, chunk), chunk)],
            dst_ref=out.at[pl.ds(pl.multiple_of(part * chunk, chunk), chunk), pl.ds(pl.multiple_of(y * cw, cw), cw)],
            send_sem=out_send.at[far, part], recv_sem=out_recv.at[far, part],
            device_id=(2 * tile + core, col), device_id_type=MESH)

    def result(far_off, carry):
        tile = lax.rem(y + 1 + far_off, plan.ys)
        near(later, tile)

        @pl.when(far_off == 0)
        def _():
            meet(now)

        def piece(part, carry):
            rows = pl.ds(pl.multiple_of(tile * h + part * chunk, chunk), chunk)
            panel[later, rows] = 1.5 * first[rows, :] - 0.75 * second[rows, :] + 0.25 * far(later, rows)
            if plan.split:
                @pl.when(far_off < plan.ys - 1)
                def _():
                    deliver(tile, far_off, part).start()
            return carry
        lax.fori_loop(0, CHUNKS, piece, 0)
        return carry
    lax.fori_loop(0, plan.ys, result, 0)

    local = pltpu.make_async_copy(
        panel.at[later, rows_of(y)],
        out.at[:, pl.ds(pl.multiple_of(y * cw if plan.split else 0, cw), cw)], out_local)
    local.start()
    sent(now)
    if plan.split:
        for far_off in range(plan.ys - 1):
            for part in range(CHUNKS):
                deliver(lax.rem(y + 1 + far_off, plan.ys), far_off, part).wait()
    local.wait()
    gather.finish()


CHUNKS = 2


def shards(row_n, col_n, matrix):
    plan = Plan(row_n, col_n, matrix.shape)
    h, half, cw = plan.h, plan.n // 2, plan.cw
    vmem = pltpu.VMEM
    count, ways = plan.ys * plan.col_n, 4 if plan.ys == 2 else 5
    shapes = [jax.ShapeDtypeStruct((h, plan.w), F32),
              jax.ShapeDtypeStruct((count * plan.total, plan.ph, plan.pw), F32)]
    if plan.halved:
        shapes.append(jax.ShapeDtypeStruct((count * plan.pieces, plan.ph, plan.pw), F32))
    spots = len(places(plan))
    turned = (2, spots, plan.ph, plan.pw) if plan.halved else (8, 128)
    return pl.pallas_call(
        functools.partial(sign_kernel, plan),
        out_shape=shapes, in_specs=[ANY], out_specs=[ANY] * len(shapes),
        scratch_shapes=[vmem((half, plan.n), BF16)] * 2 + [vmem((half, cw), BF16)] * 4
        + [vmem((2, half, cw), F32)] * 2 + [vmem((half, cw), F32)] * 2
        + [vmem((2, spots, plan.ph, plan.pw), F32), vmem(turned, F32)] + [vmem((8, 128), F32)] * 3
        + [DMA((count, plan.total)), DMA((ways,) if plan.bulk else (ways, count, plan.total)),
           DMA((count, plan.pieces)), DMA(()), DMA((2, spots)), DMA((2, spots))]
        + [DMA((2, plan.ys)), DMA((2, plan.ys)), DMA((2,)), DMA(()), DMA((plan.ys - 1, CHUNKS)),
           DMA((plan.ys - 1, CHUNKS))],
        compiler_params=pltpu.CompilerParams(collective_id=0, has_side_effects=True, vmem_limit_bytes=63 * 2**20),
        name="sign",
    )(matrix)[0]


def solution(mesh):
    body = functools.partial(shards, mesh.shape["row"], mesh.shape["col"])
    return jax.shard_map(body, mesh=mesh, in_specs=(P("row", "col"),), out_specs=P("row", "col"), check_vma=False)
```

```python
import functools

import jax
import jax.numpy as jnp
from jax import lax
from jax.experimental import pallas as pl
from jax.experimental.pallas import tpu as pltpu
from jax.sharding import PartitionSpec as P

ITERS = 2
MESH = pl.DeviceIdType.MESH
ANY = pl.BlockSpec(memory_space=pl.ANY)
DMA = pltpu.SemaphoreType.DMA
F32, BF16 = jnp.float32, jnp.bfloat16


class Plan:
    def __init__(self, row_n, col_n, block):
        self.row_n, self.col_n = row_n, col_n
        self.h, self.w = block
        self.n = self.h * row_n
        self.ys, self.zs = row_n // 2, col_n // 2
        self.q = self.h // self.w
        self.halved = self.w % 256 == 0
        self.pw = self.w // 2 if self.halved else self.w
        self.pieces = max(2, self.h * self.pw // 65536)
        self.ph = self.h // self.pieces
        self.extra = self.pw // self.ph if self.halved else 0
        self.total = self.pieces + self.extra
        self.split = (self.w // self.ys) % 128 == 0
        self.cw = self.w // self.ys if self.split else self.w
        self.bulk = self.ys == 2 and self.q % 2 == 0

    def locate(self):
        self.row, self.col = lax.axis_index("row"), lax.axis_index("col")
        self.core, self.y = lax.rem(self.row, 2), self.row // 2
        self.x, self.z = lax.rem(self.col, 2), self.col // 2

    def offset(self, row, col, piece):
        if not self.halved:
            return 0
        start = piece * self.ph
        upper = ((row * self.h + start) // self.w < col).astype(jnp.int32)
        return pl.multiple_of(self.pw * lax.rem(start // self.pw + upper, 2), self.pw)

    def place(self, row_block):
        swap = lax.rem(lax.rem(row_block, 2) + self.core, 2)
        return (swap * self.ys + row_block // 2) * self.h

    def is_mine(self, col):
        return lax.rem(col // self.q, 2) == self.core

    def is_diagonal(self, y, col):
        return col // self.q == 2 * y + self.core


def places(plan):
    ys = ((0, 0), (1, 0)) if plan.ys == 2 else ((0, 0),) + tuple(
        (far, sign) for far in range(1, plan.ys) for sign in (1, -1))
    return [(dx, dy, y_sign, z_sign) for dx in (0, 1) for dy, y_sign in ys for z_sign in (1, -1)]


class Gather:
    def __init__(self, plan, x_ref, stage, cross, put, tiles, turned, sems):
        self.plan, self.x_ref, self.stage, self.cross, self.put = plan, x_ref, stage, cross, put
        self.tiles, self.turned = tiles, turned
        self.recv, self.send, self.cross_recv, self.cross_send, self.tile_sem, self.turned_sem = sems
        row, col, x, y, z = plan.row, plan.col, plan.x, plan.y, plan.z
        self.partner = (row + 1 - 2 * plan.core, col)
        self.ways = [((row, col + 1 - 2 * x), True)]
        if plan.ys == 2:
            self.ways.append(((row + 2 - 4 * y, col), True))
        else:
            self.ways += [((row - 2, col), y > 0), ((row + 2, col), y < plan.ys - 1)]
        self.ways += [((row, col - 2), z > 0), ((row, col + 2), z < plan.zs - 1)]

    def greet(self):
        plan, barrier = self.plan, pltpu.get_barrier_semaphore()
        count = 1
        pl.semaphore_signal(barrier, inc=1, device_id=self.partner, device_id_type=MESH)
        for target, there in self.ways:
            if there is True:
                count += 1
                pl.semaphore_signal(barrier, inc=1, device_id=target, device_id_type=MESH)
            else:
                count += there.astype(jnp.int32)

                @pl.when(there)
                def _():
                    pl.semaphore_signal(barrier, inc=1, device_id=target, device_id_type=MESH)
        if plan.split and plan.ys > 2:
            count += plan.ys - 1
            for far in range(1, plan.ys):
                target = (2 * lax.rem(plan.y + far, plan.ys) + plan.core, plan.col)
                pl.semaphore_signal(barrier, inc=1, device_id=target, device_id_type=MESH)
        pl.semaphore_wait(barrier, count)

    def own(self, piece, extra=False):
        plan = self.plan
        if extra:
            start = lax.rem(plan.col, plan.q) * plan.w + (piece - plan.pieces) * plan.ph
            offset = plan.pw
        else:
            start, offset = piece * plan.ph, plan.offset(plan.row, plan.col, piece)
        return self.x_ref.at[pl.ds(pl.multiple_of(start, plan.ph), plan.ph), pl.ds(offset, plan.pw)]

    def held(self, sy, sc, piece):
        return self.stage.at[(sy * self.plan.col_n + sc) * self.plan.total + piece]

    def crossed(self, sy, sc, piece):
        return self.cross.at[(sy * self.plan.col_n + sc) * self.plan.pieces + piece]

    def link(self, act, way, src, sy, sc, piece):
        dst, at = self.held(sy, sc, piece), sy * self.plan.col_n + sc
        getattr(pltpu.make_async_remote_copy(
            src_ref=dst if src is None else src, dst_ref=dst,
            send_sem=self.send.at[way] if self.plan.bulk else self.send.at[way, at, piece],
            recv_sem=self.recv.at[at, piece], device_id=self.ways[way][0], device_id_type=MESH), act)()

    def across(self, src, sy, sc, piece):
        plan = self.plan
        if not plan.halved:
            return

        @pl.when((piece < plan.pieces) & jnp.logical_not(plan.is_mine(sc)))
        def _():
            pltpu.make_async_remote_copy(
                src_ref=self.held(sy, sc, piece) if src is None else src, dst_ref=self.crossed(sy, sc, piece),
                send_sem=self.cross_send, recv_sem=self.cross_recv.at[sy * plan.col_n + sc, piece],
                device_id=self.partner, device_id_type=MESH).start()

    def onward(self, act, src, where, piece, spot):
        plan = self.plan
        dx, dy, y_sign, z_sign = where
        sy, sc, dz = spot[:3]
        z_last = piece < plan.pieces // 4
        y_first = lax.rem(piece, 2) == 1
        near = dz == 0
        z_done = jnp.logical_or(jnp.logical_not(z_last), near)

        def go(way, when):
            there = self.ways[way][1]

            @pl.when(when if there is True else when & there)
            def _():
                self.link(act, way, src, sy, sc, piece)

        first = len(self.ways) - 2
        for way, sign in ((first, 1), (first + 1, -1)):
            here = near | (z_sign == sign)
            go(way, here if dx == 0 and dy == 0 else here & z_last)
        if dx == 0:
            go(0, z_done if dy == 0 else z_done & y_first)
        y_open = z_done if dx == 0 else z_done & jnp.logical_not(y_first)
        if plan.ys == 2:
            if dy == 0:
                go(1, y_open)
        else:
            for way, sign in ((1, 1), (2, -1)):
                if dy == 0 or y_sign == sign:
                    go(way, y_open)

    def spot(self, where, far):
        plan = self.plan
        dx, dy, y_sign, z_sign = where
        dz = far - dx - dy
        sz = plan.z + z_sign * dz
        sy = 1 - plan.y if plan.ys == 2 and dy else plan.y + y_sign * dy
        sc = 2 * sz + (1 - plan.x if dx else plan.x)
        there = (dz >= (0 if z_sign > 0 else 1)) & (sz >= 0) & (sz < plan.zs)
        if plan.ys != 2:
            there = there & (sy >= 0) & (sy < plan.ys)
        return sy, sc, dz, there, plan.is_diagonal(sy, sc) if plan.extra else None

    def has(self, spot, piece):
        there = spot[3] & (piece >= 0)
        if self.plan.extra:
            return there & ((piece < self.plan.pieces) | (spot[4] & (piece < self.plan.total)))
        return there & (piece < self.plan.total)

    def begin(self):
        plan = self.plan
        here = (0, 0, 0, 1)

        def step(extra):
            def start(piece, carry):
                src = self.own(piece, extra)
                self.onward("start", src, here, piece, (plan.y, plan.col, jnp.int32(0)))
                self.across(src, plan.y, plan.col, piece)
                return carry
            return start
        lax.fori_loop(0, plan.pieces, step(False), 0)
        if plan.extra:
            @pl.when(plan.is_diagonal(plan.y, plan.col))
            def _():
                lax.fori_loop(plan.pieces, plan.total, step(True), 0)

    def wait_arrival(self, sy, sc, piece):
        dst = self.held(sy, sc, piece)
        pltpu.make_async_remote_copy(
            src_ref=dst, dst_ref=dst, send_sem=self.send.at[0] if self.plan.bulk else self.send.at[0, 0, 0], recv_sem=self.recv.at[sy * self.plan.col_n + sc, piece],
            device_id=self.ways[0][0], device_id_type=MESH).wait_recv()

    def wait_cross(self, sy, sc, piece):
        dst = self.crossed(sy, sc, piece)
        pltpu.make_async_remote_copy(
            src_ref=dst, dst_ref=dst, send_sem=self.cross_send,
            recv_sem=self.cross_recv.at[sy * self.plan.col_n + sc, piece],
            device_id=self.partner, device_id_type=MESH).wait_recv()

    def lay(self, tile, sy, sc, piece):
        plan = self.plan
        h, w, q, ph, pw = plan.h, plan.w, plan.q, plan.ph, plan.pw
        inner = lax.rem(sc, q) * w
        row, col = piece * ph, inner + plan.offset(2 * sy + plan.core, sc, piece)
        if plan.extra:
            normal, past = piece < plan.pieces, (piece - plan.pieces) * ph
            row, col = jnp.where(normal, row, inner + past), jnp.where(normal, col, inner + pw)
        base = plan.place(sc // q)
        self.put(tile[...], sy * h + row, base + col)
        if plan.halved:
            block = ((2 * sy + plan.core) * h + row) // w

            @pl.when((plan.is_mine(sc) & (block != sc)) | jnp.logical_not(normal))
            def _():
                self.put(tile[...].T, (sc // q // 2) * h + col, sy * h + row)

    def lay_turned(self, tile, sy, sc, piece):
        plan = self.plan
        source = 2 * sy + 1 - plan.core
        at = (sc // plan.q // 2) * plan.h + lax.rem(sc, plan.q) * plan.w + plan.offset(source, sc, piece)
        self.put(tile[...].T, at, plan.place(source) + piece * plan.ph)

    def run(self):
        plan = self.plan
        wheres = places(plan)

        def fetch(act, src, slot, e):
            getattr(pltpu.make_async_copy(src, self.tiles.at[slot, e], self.tile_sem.at[slot, e]), act)()

        def fetch_turned(act, sy, sc, piece, slot, e):
            getattr(pltpu.make_async_copy(
                self.crossed(sy, sc, piece), self.turned.at[slot, e], self.turned_sem.at[slot, e]), act)()

        def arriving(far, piece, slot, e, where, spot):
            sy, sc = spot[:2]

            @pl.when(self.has(spot, piece) & (far > 0))
            def _():
                self.wait_arrival(sy, sc, piece)
                self.onward("start", None, where, piece, spot)
                self.across(None, sy, sc, piece)

            @pl.when(self.has(spot, piece - 1))
            def _():
                fetch("wait", self.held(sy, sc, piece - 1), 1 - slot, e)
                self.lay(self.tiles.at[1 - slot, e], sy, sc, piece - 1)

            @pl.when(self.has(spot, piece) & (far > 0))
            def _():
                fetch("start", self.held(sy, sc, piece), slot, e)
            if where == (0, 0, 0, 1):
                @pl.when(self.has(spot, piece) & (far == 0) & (piece < plan.pieces))
                def _():
                    fetch("start", self.own(piece), slot, e)
                if plan.extra:
                    @pl.when(self.has(spot, piece) & (far == 0) & (piece >= plan.pieces))
                    def _():
                        fetch("start", self.own(piece, True), slot, e)

        def crossing(piece, slot, e, spot):
            sy, sc = spot[:2]

            @pl.when((piece > 0) & (piece <= plan.pieces))
            def _():
                fetch_turned("wait", sy, sc, piece - 1, 1 - slot, e)
                self.lay_turned(self.turned.at[1 - slot, e], sy, sc, piece - 1)

            @pl.when(piece < plan.pieces)
            def _():
                self.wait_cross(sy, sc, piece)
                fetch_turned("start", sy, sc, piece, slot, e)

        def round_(far, carry):
            now = [self.spot(where, far) for where in wheres]
            before = [self.spot(where, far - 1) for where in wheres]

            def step(piece, carry):
                slot = lax.rem(piece, 2)
                for e, where in enumerate(wheres):
                    @pl.when(now[e][3])
                    def _():
                        arriving(far, piece, slot, e, where, now[e])
                    if plan.halved:
                        @pl.when(before[e][3] & plan.is_mine(before[e][1]))
                        def _():
                            crossing(piece, slot, e, before[e])
                return carry
            return lax.fori_loop(0, plan.total + 1, step, carry)

        lax.fori_loop(0, plan.zs + plan.ys + 1, round_, 0)

    def finish(self):
        plan = self.plan
        if plan.halved:
            some = self.cross.at[pl.ds(0, plan.ys * plan.col_n // 2 * plan.pieces)]
            pltpu.make_async_remote_copy(
                src_ref=some, dst_ref=some, send_sem=self.cross_send, recv_sem=self.cross_recv.at[0, 0],
                device_id=self.partner, device_id_type=MESH).wait_send()
        if not plan.bulk:
            def step(far, carry):
                def one(piece, carry):
                    for where in places(plan):
                        spot = self.spot(where, far)

                        @pl.when(self.has(spot, piece))
                        def _():
                            self.onward("wait_send", None, where, piece, spot)
                    return carry
                return lax.fori_loop(0, plan.total, one, carry)
            lax.fori_loop(0, plan.zs + plan.ys, step, 0)
            return

        def settle(way, count):
            some = self.stage.at[pl.ds(0, count)]
            pltpu.make_async_remote_copy(
                src_ref=some, dst_ref=some, send_sem=self.send.at[way], recv_sem=self.recv.at[0, 0],
                device_id=self.ways[way][0], device_id_type=MESH).wait_send()

        zs, last, m = plan.zs, plan.pieces // 4, plan.q // 2
        even_last, odd_last = (last + 1) // 2, last // 2
        even = (plan.pieces + 1) // 2 - even_last
        odd = plan.pieces // 2 - odd_last
        more = range(plan.pieces, plan.total)
        even_more = sum(p % 2 == 0 for p in more)
        odd_more = plan.extra - even_more
        settle(0, zs * (even + 2 * odd) + even_last + 2 * odd_last + m * (even_more + 2 * odd_more))
        settle(1, zs * (2 * even + odd) + 2 * even_last + odd_last + m * (2 * even_more + odd_more))
        each = even + odd + 4 * last
        for way, sign in ((2, 1), (3, -1)):
            marked = sum(
                ((sign * (sz - plan.z) >= 0) & (sz // m == 2 * plan.y + plan.core)).astype(jnp.int32) for sz in range(zs))
            for at in range(zs):
                spots = zs - at if sign > 0 else at + 1
                if at == (0 if sign > 0 else zs - 1):
                    continue
                for extras in range(m + 1 if plan.extra else 1):
                    @pl.when((plan.z == at) & (marked == extras if plan.extra else True))
                    def _():
                        settle(way, spots * each + extras * plan.extra)


STEPS = 8


def weights(step):
    def pick(table, other):
        value = jnp.float32(other)
        for at, entry in table:
            value = jnp.where(step == at, jnp.float32(entry), value)
        return value
    return pick(((1, 1.5),), 0.0), pick(((4, 1.5),), 0.0), pick(((1, -0.5), (4, -0.5)), 1.0)


def sign_kernel(plan, x_ref, *rest):
    if plan.halved:
        out, stage, cross = rest[:3]
        rest = rest[3:]
    else:
        out, stage = rest[:2]
        cross, rest = None, rest[2:]
    (high, low, own_high, own_low, peer_high, peer_low, panel, peer, first, second, tiles, turned, squares, peer_squares,
     scale, recv, send_sem, cross_recv, cross_send, tile_sem, turned_sem, panel_send, panel_recv, square_sems, out_local,
     out_send, out_recv) = rest
    plan.locate()
    col, core, y = plan.col, plan.core, plan.y
    h, w, q, half, cw = plan.h, plan.w, plan.q, plan.n // 2, plan.cw

    def put(tile, at, to):
        top = tile.astype(BF16)
        rest = (tile - top.astype(F32)).astype(BF16)
        rows = pl.ds(pl.multiple_of(at, tile.shape[0]), tile.shape[0])
        cols = pl.ds(pl.multiple_of(to, tile.shape[1]), tile.shape[1])
        high[rows, cols] = top
        low[rows, cols] = rest
        both = tile * tile
        squares[...] += jnp.sum(both.reshape(tile.shape[0] // 8, 8, tile.shape[1] // 128, 128), axis=(0, 2))

    gather = Gather(plan, x_ref, stage, cross, put, tiles, turned,
                    (recv, send_sem, cross_recv, cross_send, tile_sem, turned_sem))
    gather.greet()
    gather.begin()
    squares[...] = jnp.zeros_like(squares)
    gather.run()
    partner = gather.partner

    share = pltpu.make_async_remote_copy(src_ref=squares, dst_ref=peer_squares, send_sem=square_sems.at[0],
                                         recv_sem=square_sems.at[1], device_id=partner, device_id_type=MESH)
    share.start()
    share.wait()
    total = jnp.sum(jnp.sum(squares[...] + peer_squares[...], axis=0, keepdims=True), axis=1, keepdims=True)
    scale[...] = jnp.broadcast_to(jnp.sqrt(plan.n / total), scale.shape)

    def rows_of(tile):
        return pl.ds(pl.multiple_of(tile * h, h), h)

    def send(slot, tile):
        rows = rows_of(tile)
        return pltpu.make_async_remote_copy(
            src_ref=panel.at[slot, rows], dst_ref=peer.at[slot, rows], send_sem=panel_send.at[slot, tile],
            recv_sem=panel_recv.at[slot, tile], device_id=partner, device_id_type=MESH)

    def parts(value):
        top = value.astype(BF16)
        return top, (value - top.astype(F32)).astype(BF16)

    start = plan.place(col // q) + lax.rem(col, q) * w + (y * cw if plan.split else 0)
    mine_cols = pl.ds(pl.multiple_of(start, cw), cw)

    def begin(tile, carry):
        rows = rows_of(tile)
        value = scale[0:1, 0:1] * (high[rows, mine_cols].astype(F32) + low[rows, mine_cols].astype(F32))
        first[rows, :] = value
        second[rows, :] = value
        panel[0, rows] = value
        own_high[rows, :], own_low[rows, :] = parts(value)
        send(0, tile).start()
        return carry
    lax.fori_loop(0, plan.ys, begin, 0)

    def product(rows, cols, b_high, b_low):
        a_high, a_low = high[rows, cols], low[rows, cols]
        top = b_high[...]
        acc = jnp.dot(a_high, top, preferred_element_type=F32)
        acc += jnp.dot(a_high, b_low[...], preferred_element_type=F32)
        return acc + jnp.dot(a_low, top, preferred_element_type=F32)

    def near(slot, tile):
        rows = rows_of(tile)
        panel[slot, rows] = product(rows, slice(0, half), own_high, own_low)

    def far(slot, rows):
        return scale[0:1, 0:1] * (panel[slot, rows] + product(rows, slice(half, 2 * half), peer_high, peer_low))

    def meet(slot):
        for tile in range(plan.ys):
            send(slot, tile).wait_recv()
        peer_high[...], peer_low[...] = parts(peer[slot])

    def sent(slot):
        for tile in range(plan.ys):
            send(slot, tile).wait_send()

    def step_(step, carry):
        now, later = lax.rem(step, 2), lax.rem(step + 1, 2)

        @pl.when(step > 0)
        def _():
            sent(later)

        def near_(tile, carry):
            near(later, tile)
            return carry
        lax.fori_loop(0, plan.ys, near_, 0)
        meet(now)
        a, b, c = weights(step)

        def far_(tile, carry):
            rows = rows_of(tile)
            value = a * first[rows, :] + b * second[rows, :] + c * far(later, rows)
            panel[later, rows] = value
            own_high[rows, :], own_low[rows, :] = parts(value)
            send(later, tile).start()

            @pl.when(step == 1)
            def _():
                first[rows, :] = value

            @pl.when((step == 2) | (step == 5))
            def _():
                second[rows, :] = value
            return carry
        lax.fori_loop(0, plan.ys, far_, 0)
        return carry
    lax.fori_loop(0, STEPS - 1, step_, 0)

    now, later = (STEPS - 1) % 2, STEPS % 2
    chunk = h // CHUNKS
    sent(later)

    def deliver(tile, far, part):
        return pltpu.make_async_remote_copy(
            src_ref=panel.at[later, pl.ds(pl.multiple_of(tile * h + part * chunk, chunk), chunk)],
            dst_ref=out.at[pl.ds(pl.multiple_of(part * chunk, chunk), chunk), pl.ds(pl.multiple_of(y * cw, cw), cw)],
            send_sem=out_send.at[far, part], recv_sem=out_recv.at[far, part],
            device_id=(2 * tile + core, col), device_id_type=MESH)

    def result(far_off, carry):
        tile = lax.rem(y + 1 + far_off, plan.ys)
        near(later, tile)

        @pl.when(far_off == 0)
        def _():
            meet(now)

        def piece(part, carry):
            rows = pl.ds(pl.multiple_of(tile * h + part * chunk, chunk), chunk)
            panel[later, rows] = 1.5 * first[rows, :] - 0.75 * second[rows, :] + 0.25 * far(later, rows)
            if plan.split:
                @pl.when(far_off < plan.ys - 1)
                def _():
                    deliver(tile, far_off, part).start()
            return carry
        lax.fori_loop(0, CHUNKS, piece, 0)
        return carry
    lax.fori_loop(0, plan.ys, result, 0)

    local = pltpu.make_async_copy(
        panel.at[later, rows_of(y)],
        out.at[:, pl.ds(pl.multiple_of(y * cw if plan.split else 0, cw), cw)], out_local)
    local.start()
    sent(now)
    if plan.split:
        for far_off in range(plan.ys - 1):
            for part in range(CHUNKS):
                deliver(lax.rem(y + 1 + far_off, plan.ys), far_off, part).wait()
    local.wait()
    gather.finish()


CHUNKS = 2


def shards(row_n, col_n, matrix):
    plan = Plan(row_n, col_n, matrix.shape)
    h, half, cw = plan.h, plan.n // 2, plan.cw
    vmem = pltpu.VMEM
    count, ways = plan.ys * plan.col_n, 4 if plan.ys == 2 else 5
    shapes = [jax.ShapeDtypeStruct((h, plan.w), F32),
              jax.ShapeDtypeStruct((count * plan.total, plan.ph, plan.pw), F32)]
    if plan.halved:
        shapes.append(jax.ShapeDtypeStruct((count * plan.pieces, plan.ph, plan.pw), F32))
    spots = len(places(plan))
    turned = (2, spots, plan.ph, plan.pw) if plan.halved else (8, 128)
    return pl.pallas_call(
        functools.partial(sign_kernel, plan),
        out_shape=shapes, in_specs=[ANY], out_specs=[ANY] * len(shapes),
        scratch_shapes=[vmem((half, plan.n), BF16)] * 2 + [vmem((half, cw), BF16)] * 4
        + [vmem((2, half, cw), F32)] * 2 + [vmem((half, cw), F32)] * 2
        + [vmem((2, spots, plan.ph, plan.pw), F32), vmem(turned, F32)] + [vmem((8, 128), F32)] * 3
        + [DMA((count, plan.total)), DMA((ways,) if plan.bulk else (ways, count, plan.total)),
           DMA((count, plan.pieces)), DMA(()), DMA((2, spots)), DMA((2, spots))]
        + [DMA((2, plan.ys)), DMA((2, plan.ys)), DMA((2,)), DMA(()), DMA((plan.ys - 1, CHUNKS)),
           DMA((plan.ys - 1, CHUNKS))],
        compiler_params=pltpu.CompilerParams(collective_id=0, has_side_effects=True, vmem_limit_bytes=63 * 2**20),
        name="sign",
    )(matrix)[0]


def solution(mesh):
    body = functools.partial(shards, mesh.shape["row"], mesh.shape["col"])
    return jax.shard_map(body, mesh=mesh, in_specs=(P("row", "col"),), out_specs=P("row", "col"), check_vma=False)
```
